32 devices in a mesh: expert: 8 (over z, x), mp: 4 (over y, core).
Axes of the slice: x: 2, y: 2, z: 4, core: 2. Of those that a mesh axis runs over, the one named last changes fastest.
Arguments:
- tokens: bfloat16 [2048, 1024], P('expert'), may hold values from -6 to 6
- cotangent: bfloat16 [2048, 1024], P('expert'), may hold values from -6 to 6
- routes: int32 [2048, 2], P('expert'), may hold values from 0 to 7, all different within a row; in each aligned block of 256 rows (0 to 255, 256 to 511, ...) at most 96 rows name the same one
- router_weight: bfloat16 [1024, 8], replicated, may hold values from -0.1875 to 0.1875
- gate_weight: bfloat16 [8, 1024, 3584], P('expert', None, 'mp'), may hold values from -0.1875 to 0.1875
- up_weight: bfloat16 [8, 1024, 3584], P('expert', None, 'mp'), may hold values from -0.6875 to 0.6875
- down_weight: bfloat16 [8, 3584, 1024], P('expert', 'mp'), may hold values from -0.3674842 to 0.3674842
- mlp_in: float32 [3, 16], replicated, may hold values from -3.5 to 3.5
- mlp_bias: float32 [16], replicated, may hold values from -2 to 2
- mlp_out: float32 [16], replicated, may hold values from -1.5 to 1.5
Outputs:
- mixed: bfloat16 [2048, 1024], P('expert', 'mp')
- gate_update: bfloat16 [8, 1024, 3584], P('expert', None, 'mp')
- up_update: bfloat16 [8, 1024, 3584], P('expert', None, 'mp')
- down_update: bfloat16 [8, 3584, 1024], P('expert', 'mp')
- router_update: bfloat16 [1024, 8], replicated
The draws below stay inside these ranges and needn't reach their ends.
Inputs may be any that keep to these rules, and one draw needn't show every extreme that they name: `routes`: in the rows of one index of the expert axis each expert is named at most 96 times; the two experts of a row differ.
All inputs are finite; a program needn't handle non-finite values.
Results may differ from the reference program's by a relative error of at most 0.0057.
Values may be sent and summed in bfloat16 or wider, within the bound.
A program may use at most 128 MiB of HBM per device.

```python
import math
import jax
import jax.numpy as jnp
import numpy as np
from jax import lax

D = 1024
FF = 3584
TOK_DEV = 256
LOPT_UNITS = 16
FEATURES = 3
EXPERTS = 8
CAP = 96
TOKENS = 2048
N_EXPERT = 8


def draw_up_weight(key, part):
    base = jax.random.fold_in(key, 101)
    column_scale = jnp.exp(jax.random.uniform(jax.random.fold_in(base, 1), (FF,), jnp.float32, -1.15, 1.15))
    ramp = jnp.arange(EXPERTS, dtype=jnp.float32) / max(EXPERTS - 1, 1)
    entries = jnp.clip(jax.random.normal(jax.random.fold_in(base, 2), (EXPERTS, D, FF), jnp.float32), -4.0, 4.0)
    expert_scale = 3.0 ** ramp / 1.732
    values = entries * expert_scale[:, None, None] * column_scale[None, None, :] / D ** 0.5
    return values.astype(jnp.bfloat16)


def draw_down_weight(key, part):
    base = jax.random.fold_in(key, 202)
    column_scale = jnp.exp(jax.random.uniform(jax.random.fold_in(base, 1), (D,), jnp.float32, -1.15, 1.15))
    ramp = jnp.arange(EXPERTS, dtype=jnp.float32) / max(EXPERTS - 1, 1)
    entries = jnp.clip(jax.random.normal(jax.random.fold_in(base, 2), (EXPERTS, FF, D), jnp.float32), -4.0, 4.0)
    expert_scale = 3.0 ** ramp / 1.732
    values = entries * expert_scale[:, None, None] * column_scale[None, None, :] / FF ** 0.5
    return values.astype(jnp.bfloat16)


def raised(drawn, key, source, target, shards_of, factor):
    owner, partner = [(jnp.arange(drawn.shape[axis_at]) // (drawn.shape[axis_at] // shards_of)).reshape([-1 if axis == axis_at else 1 for axis in range(drawn.ndim)]) for axis_at in (source, target)]
    chosen = jax.random.permutation(key, shards_of)[partner]
    strong = (owner == chosen) | (owner == (partner + shards_of // 2) % shards_of)
    return jnp.where(strong, factor * drawn, drawn)


def levels(key, extent, pieces, least, largest):
    def one(axis_at, parts):
        heights = jax.random.uniform(jax.random.fold_in(jax.random.fold_in(key, 6), axis_at), (parts,), jnp.float32, least / len(pieces), largest / len(pieces))
        return jnp.repeat(jnp.exp(heights), extent[axis_at] // parts).reshape((-1,) + (1,) * (len(extent) - axis_at - 1))

    level = one(*pieces[0])
    for cut in pieces[1:]:
        level = level * one(*cut)
    return level


def routed_block(rng, own, number, rows, count, top, bound, lean):
    order = jax.random.permutation(rng, count)
    packed, common = shares(count, rows * top, bound, lean, True), shares(count, rows * top, bound, lean, False)
    places = jnp.arange(count)

    def named(tallies, turn):
        used = int((tallies > 0).sum())
        fixed = max(1, used // 4)
        shifted = fixed + (places - fixed + turn * (used - fixed)) % max(1, count - fixed)
        return jnp.zeros((count,), jnp.int32).at[order[jnp.where(places < fixed, places, shifted)]].set(jnp.asarray(tallies, jnp.int32))

    tallies = jnp.where(number % 4 == 0, named(packed, number // 4), named(common, number - number // 4 - 1))
    mixed = jax.random.permutation(jax.random.fold_in(own, 3), count)
    giver, sink = mixed[0:count // 2 * 2:2], mixed[1:count // 2 * 2:2]
    slack = jnp.minimum(tallies[giver] - 1, bound - tallies[sink]) // 2
    slack = jnp.where((giver == order[0]) | (sink == order[0]) | (tallies[sink] == 0), 0, jnp.maximum(slack, 0))
    shifted = jax.random.randint(jax.random.fold_in(own, 4), (count // 2,), 0, 1 << 20) % (slack + 1)
    tallies = tallies.at[giver].add(-shifted).at[sink].add(shifted)
    labels = jnp.searchsorted(jnp.cumsum(tallies), jnp.arange(rows * top), side="right").astype(jnp.int32)
    grid = labels.reshape(top, rows).T
    grid = grid[jax.random.permutation(jax.random.fold_in(own, 1), rows)]
    turn = jax.random.randint(jax.random.fold_in(own, 2), (rows, 1), 0, top)
    return jnp.take_along_axis(grid, (jnp.arange(top)[None, :] + turn) % top, axis=1)


def shares(count, total, most, slope, full):
    weights = [(1 << 20) // math.isqrt(grade ** slope) + 1 for grade in range(1, count + 1)]
    largest = most if full else min(most, max(-(-total // count), total * weights[0] // sum(weights)))
    least = 1 if total - largest >= count - 1 else 0
    given, rest = [largest] + [least] * (count - 1), total - largest - least * (count - 1)
    while rest > 0:
        movable = [i for i in range(1, count) if given[i] < largest] or [i for i in range(1, count) if given[i] < most]
        whole, budget = sum([weights[i] for i in movable]), rest
        for i in movable:
            more = min(most - given[i], max(1, budget * weights[i] // whole), rest)
            given[i] = given[i] + more
            rest = rest - more
    return np.array(given)


def centred(own_key, shape, deviation, most, cuts=(), kind=jnp.bfloat16):
    gain = levels(own_key, shape, cuts, -0.22, 0.18) if cuts else 1.0
    values = jax.random.normal(own_key, shape, jnp.float32) * deviation * gain
    return jnp.minimum(jnp.maximum(values, -most), most).astype(kind)


def heavy_noise(key, extent, spread, reach, cuts, heavy, kind=jnp.bfloat16):
    result = spread * jax.random.normal(key, extent, jnp.float32)
    if cuts:
        result = result * levels(key, extent, cuts, -0.22, 0.18)
    return jnp.clip(raised(result, jax.random.fold_in(key, 3), *heavy), -reach, reach).astype(kind)


def setup_inputs(seed: int = 0) -> dict:
    splits = jax.random.split(jax.random.key(seed), 11)
    tokens = centred(splits[0], (TOKENS, D), 1.0, 6.0, ((0, 8),))
    cotangent = heavy_noise(splits[1], (TOKENS, D), 1.0, 6.0, ((0, 8),), (0, 1, 8, 2.0))
    routes_keys = jax.random.split(jax.random.fold_in(splits[2], 1), TOKENS // TOK_DEV)
    routes_turns = jax.random.permutation(jax.random.fold_in(splits[2], 3), TOKENS // TOK_DEV)
    routes = jax.vmap(lambda own, number: routed_block(jax.random.fold_in(splits[2], 2), own, number, TOK_DEV, EXPERTS, 2, CAP, 2))(routes_keys, routes_turns).reshape((TOKENS, 2))
    router_weight = centred(splits[3], (D, EXPERTS), D ** -0.5, 0.1875)
    gate_weight = centred(splits[4], (EXPERTS, D, FF), D ** -0.5, 0.1875, ((0, 8), (2, 4)))
    up_weight = draw_up_weight(jax.random.fold_in(splits[10], 71), 0)
    down_weight = draw_down_weight(jax.random.fold_in(splits[10], 71), 0)
    mlp_in = centred(splits[7], (FEATURES, LOPT_UNITS), FEATURES ** -0.5, 3.5, (), jnp.float32)
    mlp_bias = centred(splits[8], (LOPT_UNITS,), 0.5, 2.0, (), jnp.float32)
    mlp_out = centred(splits[9], (LOPT_UNITS,), LOPT_UNITS ** -0.5, 1.5, (), jnp.float32)
    return {"tokens": tokens, "cotangent": cotangent, "routes": routes, "router_weight": router_weight, "gate_weight": gate_weight, "up_weight": up_weight, "down_weight": down_weight, "mlp_in": mlp_in, "mlp_bias": mlp_bias, "mlp_out": mlp_out}


EPSILON = 1e-06

def learned_step(gradient, weight, weight_scale, grad_rms, mlp_in, mlp_bias, mlp_out):
    feat_grad = gradient / grad_rms
    feat_weight = weight.astype(jnp.float32) * weight_scale
    feat_tanh = jnp.tanh(feat_grad)
    summed = jnp.zeros_like(feat_grad)
    for neuron in range(mlp_bias.shape[0]):
        hidden = jnp.maximum(mlp_in[0, neuron] * feat_grad + mlp_in[1, neuron] * feat_weight + mlp_in[2, neuron] * feat_tanh + mlp_bias[neuron], 0.0)
        summed = summed + mlp_out[neuron] * hidden
    return summed.astype(jnp.bfloat16)

def expert_pass(operands):
    rows_x, rows_dy, w_gate, w_up, w_down = operands
    act_gate = jnp.dot(rows_x, w_gate, preferred_element_type=jnp.float32)
    act_up = jnp.dot(rows_x, w_up, preferred_element_type=jnp.float32)
    sigmoid_gate = jax.nn.sigmoid(act_gate)
    silu_gate = act_gate * sigmoid_gate
    hidden = (silu_gate * act_up).astype(jnp.bfloat16)
    expert_out = jnp.dot(hidden, w_down, preferred_element_type=jnp.float32).astype(jnp.bfloat16)
    grad_down = jnp.dot(hidden.T, rows_dy, preferred_element_type=jnp.float32)
    grad_hidden = jnp.dot(rows_dy, w_down.T, preferred_element_type=jnp.float32)
    d_gate = (grad_hidden * act_up * sigmoid_gate * (1.0 + act_gate * (1.0 - sigmoid_gate))).astype(jnp.bfloat16)
    d_up = (grad_hidden * silu_gate).astype(jnp.bfloat16)
    grad_gate = jnp.dot(rows_x.T, d_gate, preferred_element_type=jnp.float32)
    grad_up = jnp.dot(rows_x.T, d_up, preferred_element_type=jnp.float32)
    return (expert_out, grad_gate, grad_up, grad_down)

def reference(tokens, cotangent, routes, router_weight, gate_weight, up_weight, down_weight, mlp_in, mlp_bias, mlp_out):
    expert_ids = jnp.arange(EXPERTS, dtype=jnp.int32)
    picks = (routes[:, :, None] == expert_ids[None, None, :]).astype(jnp.int32)
    blocks = picks.reshape(N_EXPERT, TOK_DEV * 2, EXPERTS)
    before = jnp.cumsum(blocks, axis=1) - blocks
    places = lax.optimization_barrier(jnp.sum(before * blocks, axis=2)).reshape(TOKENS, 2).astype(jnp.int32)
    sources = (jnp.arange(TOKENS, dtype=jnp.int32) // TOK_DEV)[:, None]
    slot_rows = (sources * CAP + places).astype(jnp.int32)
    chosen = picks.astype(jnp.float32)
    logits = jnp.dot(tokens, router_weight, preferred_element_type=jnp.float32)
    picked = lax.optimization_barrier(jnp.sum(logits[:, None, :] * chosen, axis=2))
    sigmas = jax.nn.sigmoid(picked)
    denominator = lax.optimization_barrier(jnp.sum(sigmas, axis=1, keepdims=True))
    gates = sigmas / denominator
    scaled_cot = (gates[:, :, None] * cotangent.astype(jnp.float32)[:, None, :]).astype(jnp.bfloat16)
    flat_experts = routes.reshape(-1).astype(jnp.int32)
    flat_rows = slot_rows.reshape(-1)
    x_in = jnp.zeros((EXPERTS, EXPERTS * CAP, D), jnp.bfloat16).at[flat_experts, flat_rows].set(jnp.repeat(tokens, 2, axis=0))
    dy_in = jnp.zeros((EXPERTS, EXPERTS * CAP, D), jnp.bfloat16).at[flat_experts, flat_rows].set(scaled_cot.reshape(TOKENS * 2, D))
    expert_out, grad_gate, grad_up, grad_down = lax.map(expert_pass, (x_in, dy_in, gate_weight, up_weight, down_weight))
    routed = expert_out[flat_experts, flat_rows].astype(jnp.float32).reshape(TOKENS, 2, D)
    mixed = (tokens.astype(jnp.float32) + gates[:, 0:1] * routed[:, 0] + gates[:, 1:2] * routed[:, 1]).astype(jnp.bfloat16)
    gate_grads = lax.optimization_barrier(jnp.sum(cotangent.astype(jnp.float32)[:, None, :] * routed, axis=2))
    mean_part = lax.optimization_barrier(jnp.sum(gates * gate_grads, axis=1, keepdims=True))
    sigma_grads = (gate_grads - mean_part) / denominator
    logit_grads = sigma_grads * sigmas * (1.0 - sigmas)
    dense_grads = lax.optimization_barrier(jnp.sum(logit_grads[:, :, None] * chosen, axis=1)).astype(jnp.bfloat16)
    router_grad = jnp.dot(tokens.T, dense_grads, preferred_element_type=jnp.float32)
    total_count = EXPERTS * D * FF
    gate_rms = jnp.sqrt(jnp.sum(grad_gate * grad_gate) / total_count + EPSILON)
    up_rms = jnp.sqrt(jnp.sum(grad_up * grad_up) / total_count + EPSILON)
    down_rms = jnp.sqrt(jnp.sum(grad_down * grad_down) / total_count + EPSILON)
    router_rms = jnp.sqrt(jnp.sum(router_grad * router_grad) / (D * EXPERTS) + EPSILON)

    def expert_updates(operands):
        g_gate, g_up, g_down, w_gate, w_up, w_down = operands
        return (learned_step(g_gate, w_gate, D ** 0.5, gate_rms, mlp_in, mlp_bias, mlp_out), learned_step(g_up, w_up, D ** 0.5, up_rms, mlp_in, mlp_bias, mlp_out), learned_step(g_down, w_down, FF ** 0.5, down_rms, mlp_in, mlp_bias, mlp_out))
    gate_update, up_update, down_update = lax.map(expert_updates, (grad_gate, grad_up, grad_down, gate_weight, up_weight, down_weight))
    router_update = learned_step(router_grad, router_weight, D ** 0.5, router_rms, mlp_in, mlp_bias, mlp_out)
    return (mixed, gate_update, up_update, down_update, router_update)
```

```python
import functools

import jax
import jax.numpy as jnp
from jax import lax
from jax.experimental import pallas as pl
from jax.experimental.pallas import tpu as pltpu
from jax.sharding import PartitionSpec as P

EPSILON = 1e-06
MESH = pl.DeviceIdType.MESH


def dispatch_kernel(n, groups, colw, send_ref, out_ref, loc, s1, r1, ls, lr, hs, hr, fs, fr):
    me = lax.axis_index("expert")
    col = lax.axis_index("mp")
    partner = col + 1 - 2 * lax.rem(col, 2)
    highs = groups // 2
    barrier = pltpu.get_barrier_semaphore()

    def greet(i, _):
        pl.semaphore_signal(
            barrier, inc=1, device_id=(lax.rem(me + i, n), col), device_id_type=MESH
        )
        return 0

    lax.fori_loop(1, n, greet, 0)
    pl.semaphore_signal(barrier, inc=1, device_id=(me, partner), device_id_type=MESH)
    for h in range(1, highs):
        pl.semaphore_signal(
            barrier, inc=1, device_id=(me, lax.rem(col + 2 * h, groups)), device_id_type=MESH
        )
    pl.semaphore_wait(barrier, n - 1 + 1 + highs - 1)

    def cols(c):
        return pl.ds(pl.multiple_of(c * colw, 128), colw)

    def spread(i):
        peer = lax.rem(me + i, n)
        return pltpu.make_async_remote_copy(
            src_ref=send_ref.at[:, peer],
            dst_ref=out_ref.at[:, me, :, cols(col)],
            send_sem=s1.at[i],
            recv_sem=r1.at[i],
            device_id=(peer, col),
            device_id_type=MESH,
        )

    def block(owner, i):
        return out_ref.at[:, lax.rem(me - i + n, n), :, cols(owner)]

    def to(owner, i, send, recv, target):
        ref = block(owner, i)
        return pltpu.make_async_remote_copy(
            src_ref=ref,
            dst_ref=ref,
            send_sem=send,
            recv_sem=recv,
            device_id=(me, target),
            device_id_type=MESH,
        )

    def low(i):
        return to(col, i, ls.at[i], lr.at[i], partner)

    def high(h, i):
        return to(col, i, hs.at[h - 1, i], hr.at[h - 1, i], lax.rem(col + 2 * h, groups))

    def forward(h, i):
        owner = lax.rem(col - 2 * h + 2 * groups, groups)
        return to(owner, i, fs.at[h - 1, i], fr.at[h - 1, i], partner)

    own = pltpu.make_async_copy(send_ref.at[:, me], out_ref.at[:, me, :, cols(col)], loc)
    own.start()

    def start(i, _):
        spread(i).start()
        return 0

    lax.fori_loop(1, n, start, 0)
    own.wait()

    def share(i):
        for h in range(1, highs):
            high(h, i).start()
        low(i).start()

    def relay(i):
        for h in range(1, highs):
            high(h, i).wait_recv()
            forward(h, i).start()

    share(0)

    def step(i, _):
        spread(i).wait_recv()
        share(i)
        relay(i - 1)
        return 0

    lax.fori_loop(1, n, step, 0)
    relay(n - 1)

    def finish(i, _):
        low(i).wait()
        for h in range(1, highs):
            high(h, i).wait_send()
            forward(h, i).wait()
        return 0

    def finish_spread(i, _):
        spread(i).wait_send()
        return 0

    lax.fori_loop(0, n, finish, 0)
    lax.fori_loop(1, n, finish_spread, 0)


def dispatch(send, n, groups):
    _, _, cap, colw = send.shape
    dma = pltpu.SemaphoreType.DMA
    highs = max(groups // 2 - 1, 1)
    return pl.pallas_call(
        functools.partial(dispatch_kernel, n, groups, colw),
        out_shape=jax.ShapeDtypeStruct((2, n, cap, colw * groups), send.dtype),
        in_specs=[pl.BlockSpec(memory_space=pltpu.VMEM)],
        out_specs=pl.BlockSpec(memory_space=pltpu.VMEM),
        scratch_shapes=[
            dma,
            dma((n,)),
            dma((n,)),
            dma((n,)),
            dma((n,)),
            dma((highs, n)),
            dma((highs, n)),
            dma((highs, n)),
            dma((highs, n)),
        ],
        compiler_params=pltpu.CompilerParams(collective_id=0, has_side_effects=True),
        name="dispatch",
    )(send)


def gather_all_kernel(n, groups, x_ref, out_ref, loc, ss, rs):
    total = n * groups
    me = lax.axis_index("expert") * groups + lax.axis_index("mp")
    barrier = pltpu.get_barrier_semaphore()

    def place(i):
        peer = lax.rem(me + i, total)
        return (peer // groups, lax.rem(peer, groups))

    def greet(i, _):
        pl.semaphore_signal(barrier, inc=1, device_id=place(i), device_id_type=MESH)
        return 0

    own = pltpu.make_async_copy(x_ref, out_ref.at[me], loc)
    own.start()
    lax.fori_loop(1, total, greet, 0)
    pl.semaphore_wait(barrier, total - 1)

    def copy(i):
        return pltpu.make_async_remote_copy(
            src_ref=x_ref,
            dst_ref=out_ref.at[me],
            send_sem=ss.at[i],
            recv_sem=rs.at[i],
            device_id=place(i),
            device_id_type=MESH,
        )

    def start(i, _):
        copy(i).start()
        return 0

    def finish(i, _):
        copy(i).wait()
        return 0

    lax.fori_loop(1, total, start, 0)
    own.wait()
    lax.fori_loop(1, total, finish, 0)


def gather_all(x, n, groups):
    total = n * groups
    return pl.pallas_call(
        functools.partial(gather_all_kernel, n, groups),
        out_shape=jax.ShapeDtypeStruct((total,) + x.shape, x.dtype),
        in_specs=[pl.BlockSpec(memory_space=pltpu.VMEM)],
        out_specs=pl.BlockSpec(memory_space=pltpu.VMEM),
        scratch_shapes=[
            pltpu.SemaphoreType.DMA,
            pltpu.SemaphoreType.DMA((total,)),
            pltpu.SemaphoreType.DMA((total,)),
        ],
        compiler_params=pltpu.CompilerParams(collective_id=1, has_side_effects=True),
        name="gather_all",
    )(x)


def gather_experts_kernel(n, x_ref, out_ref, buf, loc, ss, rs):
    me = lax.axis_index("expert")
    col = lax.axis_index("mp")
    barrier = pltpu.get_barrier_semaphore()

    def greet(i, _):
        pl.semaphore_signal(
            barrier, inc=1, device_id=(lax.rem(me + i, n), col), device_id_type=MESH
        )
        return 0

    own = pltpu.make_async_copy(x_ref, buf.at[me], loc)
    own.start()
    lax.fori_loop(1, n, greet, 0)
    pl.semaphore_wait(barrier, n - 1)

    def copy(i):
        return pltpu.make_async_remote_copy(
            src_ref=x_ref,
            dst_ref=buf.at[me],
            send_sem=ss.at[i],
            recv_sem=rs.at[i],
            device_id=(lax.rem(me + i, n), col),
            device_id_type=MESH,
        )

    def start(i, _):
        copy(i).start()
        return 0

    def finish(i, _):
        copy(i).wait()
        return 0

    lax.fori_loop(1, n, start, 0)
    own.wait()
    lax.fori_loop(1, n, finish, 0)
    out_ref[...] = buf[0]

    def add(i, _):
        out_ref[...] += buf[i]
        return 0

    lax.fori_loop(1, n, add, 0)


def sum_experts(x, n):
    return pl.pallas_call(
        functools.partial(gather_experts_kernel, n),
        out_shape=jax.ShapeDtypeStruct(x.shape, x.dtype),
        in_specs=[pl.BlockSpec(memory_space=pltpu.VMEM)],
        out_specs=pl.BlockSpec(memory_space=pltpu.VMEM),
        scratch_shapes=[
            pltpu.VMEM((n,) + x.shape, x.dtype),
            pltpu.SemaphoreType.DMA,
            pltpu.SemaphoreType.DMA((n,)),
            pltpu.SemaphoreType.DMA((n,)),
        ],
        compiler_params=pltpu.CompilerParams(collective_id=2, has_side_effects=True),
        name="sum_experts",
    )(x)


def update_kernel(units, chunk, coef_ref, g_ref, w_ref, out_ref):
    rows, width = g_ref.shape
    strips = width // 128

    def body(step, _):
        r = pl.ds(pl.multiple_of((step // strips) * chunk, chunk), chunk)
        c = pl.ds(pl.multiple_of(lax.rem(step, strips) * 128, 128), 128)

        def coef(i):
            return jnp.concatenate([coef_ref[i]] * (chunk // 8), axis=0)

        f0 = g_ref[r, c] * coef(5 * units)
        f1 = w_ref[r, c].astype(jnp.float32)
        f2 = jnp.tanh(f0)
        acc = coef(5 * units + 1)
        for j in range(units):
            y = coef(j) * f0 + coef(units + j) * f1 + coef(2 * units + j) * f2
            acc = acc + coef(4 * units + j) * jnp.maximum(y, coef(3 * units + j))
        out_ref[r, c] = acc.astype(jnp.bfloat16)
        return 0

    lax.fori_loop(0, (rows // chunk) * strips, body, 0)


def update(g, w, scale, rms, mlp_in, mlp_bias, mlp_out):
    units = mlp_bias.shape[0]
    table = jnp.concatenate(
        [
            mlp_in[0],
            mlp_in[1] * scale,
            mlp_in[2],
            -mlp_bias,
            mlp_out,
            (1.0 / rms)[None],
            jnp.sum(mlp_out * mlp_bias)[None],
        ]
    )
    table = jnp.broadcast_to(table[:, None, None], (table.shape[0], 8, 128))
    rows, width = g.shape
    chunk = 64 if rows % 64 == 0 else rows
    steps = 4 if rows % (4 * chunk) == 0 else 2 if rows % (2 * chunk) == 0 else 1
    if chunk < 64:
        chunk = 8
    block = rows // steps
    return pl.pallas_call(
        functools.partial(update_kernel, units, chunk),
        grid=(steps,),
        out_shape=jax.ShapeDtypeStruct((rows, width), jnp.bfloat16),
        in_specs=[
            pl.BlockSpec(table.shape, lambda i: (0, 0, 0)),
            pl.BlockSpec((block, width), lambda i: (i, 0)),
            pl.BlockSpec((block, width), lambda i: (i, 0)),
        ],
        out_specs=pl.BlockSpec((block, width), lambda i: (i, 0)),
        cost_estimate=pl.CostEstimate(
            flops=rows * width * 9 * units, bytes_accessed=rows * width * 8, transcendentals=rows * width
        ),
        name="update",
    )(table, g, w)


def route_tables(routes, experts, capacity):
    chosen = (routes[:, :, None] == jnp.arange(experts, dtype=jnp.int32)[None, None, :]).astype(
        jnp.int32
    )
    flat_picks = chosen.reshape(-1, experts)
    before = jnp.cumsum(flat_picks, axis=0) - flat_picks
    places = jnp.sum(before * flat_picks, axis=1).reshape(routes.shape)
    slot_hit = (places[:, :, None] == jnp.arange(capacity, dtype=jnp.int32)[None, None, :]).astype(
        jnp.bfloat16
    )
    mover = chosen.astype(jnp.bfloat16)[:, :, :, None] * slot_hit[:, :, None, :]
    return (chosen.astype(jnp.float32), mover)


def on_device(
    tokens,
    cotangent,
    routes,
    router_weight,
    gate_weight,
    up_weight,
    down_weight,
    mlp_in,
    mlp_bias,
    mlp_out,
):
    experts = lax.axis_size("expert")
    groups = lax.axis_size("mp")
    tok_count = tokens.shape[0]
    capacity = 3 * tok_count // experts
    width = tokens.shape[1]
    col_width = width // groups
    mp = lax.axis_index("mp")
    me = lax.axis_index("expert")
    col_start = mp * col_width
    chosen, mover = route_tables(routes, experts, capacity)
    logits = jnp.dot(tokens, router_weight, preferred_element_type=jnp.float32)
    picked = jnp.sum(logits[:, None, :] * chosen, axis=2)
    sigmas = jax.nn.sigmoid(picked)
    denominator = jnp.sum(sigmas, axis=1, keepdims=True)
    gates = sigmas / denominator
    token_cols = lax.dynamic_slice_in_dim(tokens, col_start, col_width, 1)
    cot_cols = lax.dynamic_slice_in_dim(cotangent, col_start, col_width, 1)
    scaled_cot = (gates[:, :, None] * cot_cols.astype(jnp.float32)[:, None, :]).astype(
        jnp.bfloat16
    )
    send_x = jnp.einsum(
        "tkec,td->ecd", mover, token_cols, preferred_element_type=jnp.float32
    ).astype(jnp.bfloat16)
    send_dy = jnp.einsum(
        "tkec,tkd->ecd", mover, scaled_cot, preferred_element_type=jnp.float32
    ).astype(jnp.bfloat16)
    got = dispatch(jnp.stack([send_x, send_dy]), experts, groups)
    slots = experts * capacity
    rows_x = got[0].reshape(slots, width)
    rows_dy = got[1].reshape(slots, width)
    w_gate = gate_weight[0]
    w_up = up_weight[0]
    w_down = down_weight[0]
    hidden_units = w_gate.shape[1] * groups
    act_gate = jnp.dot(rows_x, w_gate, preferred_element_type=jnp.float32)
    act_up = jnp.dot(rows_x, w_up, preferred_element_type=jnp.float32)
    sigmoid_gate = jax.nn.sigmoid(act_gate)
    silu_gate = act_gate * sigmoid_gate
    hidden = (silu_gate * act_up).astype(jnp.bfloat16)
    partial_out = jnp.dot(hidden, w_down, preferred_element_type=jnp.float32).astype(jnp.bfloat16)
    total_out = lax.dynamic_slice_in_dim(partial_out, col_start, col_width, 1).astype(jnp.float32)
    for shift in range(1, groups):
        target = lax.rem(mp + shift, groups)
        piece = lax.dynamic_slice_in_dim(partial_out, target * col_width, col_width, 1)
        moved = lax.ppermute(piece, "mp", [(m, (m + shift) % groups) for m in range(groups)])
        total_out = total_out + moved.astype(jnp.float32)
    back_rows = total_out.astype(jnp.bfloat16).reshape(experts, capacity, col_width)
    returned = lax.all_to_all(back_rows, "expert", split_axis=0, concat_axis=0, tiled=True)

    grad_down = jnp.einsum("sf,sd->fd", hidden, rows_dy, preferred_element_type=jnp.float32)
    grad_hidden = jnp.einsum("sd,fd->sf", rows_dy, w_down, preferred_element_type=jnp.float32)
    d_gate = (grad_hidden * act_up * sigmoid_gate * (1.0 + act_gate * (1.0 - sigmoid_gate))).astype(
        jnp.bfloat16
    )
    d_up = (grad_hidden * silu_gate).astype(jnp.bfloat16)
    inner = jnp.sum(grad_hidden * hidden.astype(jnp.float32), axis=1)
    grad_gate = jnp.einsum("sd,sf->df", rows_x, d_gate, preferred_element_type=jnp.float32)
    grad_up = jnp.einsum("sd,sf->df", rows_x, d_up, preferred_element_type=jnp.float32)

    norms = jnp.stack(
        [
            jnp.sum(grad_gate * grad_gate),
            jnp.sum(grad_up * grad_up),
            jnp.sum(grad_down * grad_down),
        ]
    )
    need = slots + 3
    lines = -(-need // 1024) * 8
    parcel = jnp.concatenate([inner, norms, jnp.zeros((lines * 128 - need,), jnp.float32)])
    parcels = gather_all(parcel.reshape(lines, 128), experts, groups)
    parcels = jnp.sum(parcels.reshape(experts, groups, lines * 128), axis=1)
    norm_sums = jnp.sum(parcels[:, slots : slots + 3], axis=0)
    inner_own = lax.dynamic_slice(parcels, (0, me * capacity), (experts, capacity))

    total_count = experts * width * hidden_units
    rms = jnp.sqrt(norm_sums / total_count + EPSILON)
    net = (mlp_in, mlp_bias, mlp_out)
    gate_update = update(grad_gate, w_gate, width**0.5, rms[0], *net)[None]
    up_update = update(grad_up, w_up, width**0.5, rms[1], *net)[None]
    down_update = update(grad_down, w_down, hidden_units**0.5, rms[2], *net)[None]

    gated = jnp.sum(mover.astype(jnp.float32) * inner_own[None, None], axis=(2, 3))
    logit_grads = (gated - gates * jnp.sum(gated, axis=1, keepdims=True)) * (1.0 - sigmas)
    dense_grads = jnp.sum(logit_grads[:, :, None] * chosen, axis=1).astype(jnp.bfloat16)
    router_part = jnp.einsum("te,td->ed", dense_grads, tokens, preferred_element_type=jnp.float32)
    router_grad = sum_experts(router_part, experts)
    router_rms = jnp.sqrt(jnp.sum(router_grad * router_grad) / (width * experts) + EPSILON)
    router_update = update(router_grad, router_weight.T, width**0.5, router_rms, *net).T

    routed = jnp.einsum("tkec,ecd->tkd", mover, returned, preferred_element_type=jnp.float32)
    mixed = (
        token_cols.astype(jnp.float32) + gates[:, 0:1] * routed[:, 0] + gates[:, 1:2] * routed[:, 1]
    ).astype(jnp.bfloat16)
    return (mixed, gate_update, up_update, down_update, router_update)


def solution(mesh):
    placed = (
        P("expert", None),
        P("expert", None),
        P("expert", None),
        P(),
        P("expert", None, "mp"),
        P("expert", None, "mp"),
        P("expert", "mp", None),
        P(),
        P(),
        P(),
    )
    return jax.shard_map(
        on_device,
        mesh=mesh,
        in_specs=placed,
        out_specs=(
            P("expert", "mp"),
            P("expert", None, "mp"),
            P("expert", None, "mp"),
            P("expert", "mp", None),
            P(),
        ),
        check_vma=False,
    )
```

```python
import functools

import jax
import jax.numpy as jnp
from jax import lax
from jax.experimental import pallas as pl
from jax.experimental.pallas import tpu as pltpu
from jax.sharding import PartitionSpec as P

EPSILON = 1e-06
CHUNK = 128
MESH = pl.DeviceIdType.MESH


def dispatch_kernel(n, groups, colw, send_ref, out_ref, loc, s1, r1, ls, lr, hs, hr, fs, fr):
    me = lax.axis_index("expert")
    col = lax.axis_index("mp")
    partner = col + 1 - 2 * lax.rem(col, 2)
    highs = groups // 2
    barrier = pltpu.get_barrier_semaphore()

    def greet(i, _):
        pl.semaphore_signal(
            barrier, inc=1, device_id=(lax.rem(me + i, n), col), device_id_type=MESH
        )
        return 0

    lax.fori_loop(1, n, greet, 0)
    pl.semaphore_signal(barrier, inc=1, device_id=(me, partner), device_id_type=MESH)
    for h in range(1, highs):
        pl.semaphore_signal(
            barrier, inc=1, device_id=(me, lax.rem(col + 2 * h, groups)), device_id_type=MESH
        )
    pl.semaphore_wait(barrier, n - 1 + 1 + highs - 1)

    def cols(c):
        return pl.ds(pl.multiple_of(c * colw, 128), colw)

    def spread(i):
        peer = lax.rem(me + i, n)
        return pltpu.make_async_remote_copy(
            src_ref=send_ref.at[:, peer],
            dst_ref=out_ref.at[:, me, :, cols(col)],
            send_sem=s1.at[i],
            recv_sem=r1.at[i],
            device_id=(peer, col),
            device_id_type=MESH,
        )

    def block(owner, i):
        return out_ref.at[:, lax.rem(me - i + n, n), :, cols(owner)]

    def to(owner, i, send, recv, target):
        ref = block(owner, i)
        return pltpu.make_async_remote_copy(
            src_ref=ref,
            dst_ref=ref,
            send_sem=send,
            recv_sem=recv,
            device_id=(me, target),
            device_id_type=MESH,
        )

    def low(i):
        return to(col, i, ls.at[i], lr.at[i], partner)

    def high(h, i):
        return to(col, i, hs.at[h - 1, i], hr.at[h - 1, i], lax.rem(col + 2 * h, groups))

    def forward(h, i):
        owner = lax.rem(col - 2 * h + 2 * groups, groups)
        return to(owner, i, fs.at[h - 1, i], fr.at[h - 1, i], partner)

    own = pltpu.make_async_copy(send_ref.at[:, me], out_ref.at[:, me, :, cols(col)], loc)
    own.start()

    def start(i, _):
        spread(i).start()
        return 0

    lax.fori_loop(1, n, start, 0)
    own.wait()

    def share(i):
        for h in range(1, highs):
            high(h, i).start()
        low(i).start()

    def relay(i):
        for h in range(1, highs):
            high(h, i).wait_recv()
            forward(h, i).start()

    share(0)

    def step(i, _):
        spread(i).wait_recv()
        share(i)
        relay(i - 1)
        return 0

    lax.fori_loop(1, n, step, 0)
    relay(n - 1)

    def finish(i, _):
        low(i).wait()
        for h in range(1, highs):
            high(h, i).wait_send()
            forward(h, i).wait()
        return 0

    def finish_spread(i, _):
        spread(i).wait_send()
        return 0

    lax.fori_loop(0, n, finish, 0)
    lax.fori_loop(1, n, finish_spread, 0)


def dispatch(send, n, groups):
    _, _, cap, colw = send.shape
    dma = pltpu.SemaphoreType.DMA
    highs = max(groups // 2 - 1, 1)
    return pl.pallas_call(
        functools.partial(dispatch_kernel, n, groups, colw),
        out_shape=jax.ShapeDtypeStruct((2, n, cap, colw * groups), send.dtype),
        in_specs=[pl.BlockSpec(memory_space=pltpu.VMEM)],
        out_specs=pl.BlockSpec(memory_space=pltpu.VMEM),
        scratch_shapes=[
            dma,
            dma((n,)),
            dma((n,)),
            dma((n,)),
            dma((n,)),
            dma((highs, n)),
            dma((highs, n)),
            dma((highs, n)),
            dma((highs, n)),
        ],
        compiler_params=pltpu.CompilerParams(collective_id=0, has_side_effects=True),
        name="dispatch",
    )(send)


def gather_sums_kernel(n, groups, x_ref, out_ref, parts, mine, ms, mr, es, er):
    me = lax.axis_index("expert")
    col = lax.axis_index("mp")
    barrier = pltpu.get_barrier_semaphore()

    def greet_mp(i, _):
        pl.semaphore_signal(
            barrier, inc=1, device_id=(me, lax.rem(col + i, groups)), device_id_type=MESH
        )
        return 0

    def greet(i, _):
        pl.semaphore_signal(
            barrier, inc=1, device_id=(lax.rem(me + i, n), col), device_id_type=MESH
        )
        return 0

    lax.fori_loop(1, groups, greet_mp, 0)
    lax.fori_loop(1, n, greet, 0)
    parts[col] = x_ref[...]
    pl.semaphore_wait(barrier, groups - 1 + n - 1)

    def across(i):
        return pltpu.make_async_remote_copy(
            src_ref=x_ref,
            dst_ref=parts.at[col],
            send_sem=ms.at[i],
            recv_sem=mr.at[i],
            device_id=(me, lax.rem(col + i, groups)),
            device_id_type=MESH,
        )

    def spread(i):
        return pltpu.make_async_remote_copy(
            src_ref=mine,
            dst_ref=out_ref.at[me],
            send_sem=es.at[i],
            recv_sem=er.at[i],
            device_id=(lax.rem(me + i, n), col),
            device_id_type=MESH,
        )

    def start_across(i, _):
        across(i).start()
        return 0

    def finish_across(i, _):
        across(i).wait()
        return 0

    def start(i, _):
        spread(i).start()
        return 0

    def finish(i, _):
        spread(i).wait()
        return 0

    lax.fori_loop(1, groups, start_across, 0)
    lax.fori_loop(1, groups, finish_across, 0)
    total = parts[0]
    for i in range(1, groups):
        total = total + parts[i]
    mine[...] = total
    out_ref[me] = total
    lax.fori_loop(1, n, start, 0)
    lax.fori_loop(1, n, finish, 0)


def gather_sums(x, n, groups):
    dma = pltpu.SemaphoreType.DMA
    return pl.pallas_call(
        functools.partial(gather_sums_kernel, n, groups),
        out_shape=jax.ShapeDtypeStruct((n,) + x.shape, x.dtype),
        in_specs=[pl.BlockSpec(memory_space=pltpu.VMEM)],
        out_specs=pl.BlockSpec(memory_space=pltpu.VMEM),
        scratch_shapes=[
            pltpu.VMEM((groups,) + x.shape, x.dtype),
            pltpu.VMEM(x.shape, x.dtype),
            dma((groups,)),
            dma((groups,)),
            dma((n,)),
            dma((n,)),
        ],
        compiler_params=pltpu.CompilerParams(collective_id=1, has_side_effects=True),
        name="gather_sums",
    )(x)


def update_kernel(units, chunk, scale, inv_ref, coef_ref, g_ref, w_ref, out_ref):
    rows, width = g_ref.shape
    strips = width // 128
    inv = inv_ref[0]

    def body(step, _):
        r = pl.ds(pl.multiple_of((step // strips) * chunk, chunk), chunk)
        c = pl.ds(pl.multiple_of(lax.rem(step, strips) * 128, 128), 128)

        def coef(i):
            return jnp.concatenate([coef_ref[i]] * (chunk // 8), axis=0)

        f0 = g_ref[r, c] * inv
        f1 = w_ref[r, c].astype(jnp.float32) * scale
        f2 = jnp.tanh(f0)
        acc = coef(5 * units)
        for j in range(units):
            y = coef(j) * f0 + coef(units + j) * f1 + coef(2 * units + j) * f2
            acc = acc + coef(4 * units + j) * jnp.maximum(y, coef(3 * units + j))
        out_ref[r, c] = acc.astype(jnp.bfloat16)
        return 0

    lax.fori_loop(0, (rows // chunk) * strips, body, 0)


def update_send_kernel(
    units, chunk, scale, n, inv_ref, coef_ref, g_ref, w_ref, part_ref, rows_ref, out_ref, total_ref, back_ref, parts, returned, outgoing, ls, ps, pr, qs, qr
):
    me = lax.axis_index("expert")
    col = lax.axis_index("mp")
    step = pl.program_id(0)

    def part(i):
        return pltpu.make_async_remote_copy(
            src_ref=parts.at[me],
            dst_ref=parts.at[me],
            send_sem=ps.at[i],
            recv_sem=pr.at[i],
            device_id=(lax.rem(me + i, n), col),
            device_id_type=MESH,
        )

    def back(i):
        peer = lax.rem(me + i, n)
        return pltpu.make_async_remote_copy(
            src_ref=outgoing.at[peer],
            dst_ref=returned.at[me],
            send_sem=qs.at[i],
            recv_sem=qr.at[i],
            device_id=(peer, col),
            device_id_type=MESH,
        )

    def own():
        return (
            pltpu.make_async_copy(part_ref, parts.at[me], ls.at[0]),
            pltpu.make_async_copy(rows_ref.at[me], returned.at[me], ls.at[1]),
            pltpu.make_async_copy(rows_ref, outgoing, ls.at[2]),
        )

    @pl.when(step == 0)
    def _():
        barrier = pltpu.get_barrier_semaphore()

        def greet(i, _):
            pl.semaphore_signal(
                barrier, inc=1, device_id=(lax.rem(me + i, n), col), device_id_type=MESH
            )
            return 0

        lax.fori_loop(1, n, greet, 0)
        for copy in own():
            copy.start()
        for copy in own():
            copy.wait()
        pl.semaphore_wait(barrier, n - 1)

        def start(i, _):
            part(i).start()
            back(i).start()
            return 0

        lax.fori_loop(1, n, start, 0)

    update_kernel(units, chunk, scale, inv_ref, coef_ref, g_ref, w_ref, out_ref)

    @pl.when(step == pl.num_programs(0) - 1)
    def _():
        def finish(i, _):
            part(i).wait()
            back(i).wait()
            return 0

        lax.fori_loop(1, n, finish, 0)
        total_ref[...] = parts[0]

        def add(i, _):
            total_ref[...] += parts[i]
            return 0

        lax.fori_loop(1, n, add, 0)
        back_ref[...] = returned[...]


def network_table(mlp_in, mlp_bias, mlp_out):
    rows = jnp.concatenate(
        [mlp_in.reshape(-1), -mlp_bias, mlp_out, jnp.sum(mlp_out * mlp_bias)[None]]
    )
    return jnp.broadcast_to(rows[:, None, None], (rows.shape[0], 8, 128))


def update(g, w, scale, rms, table, send=None):
    units = table.shape[0] // 5
    inv = (1.0 / rms).reshape(1)
    rows, width = g.shape
    chunk = CHUNK if rows % CHUNK == 0 else rows
    steps = 4 if rows % (4 * chunk) == 0 else 2 if rows % (2 * chunk) == 0 else 1
    if chunk == rows:
        chunk = 8
    block = rows // steps
    in_specs = [
        pl.BlockSpec(memory_space=pltpu.SMEM),
        pl.BlockSpec(table.shape, lambda i: (0, 0, 0)),
        pl.BlockSpec((block, width), lambda i: (i, 0)),
        pl.BlockSpec((block, width), lambda i: (i, 0)),
    ]
    out_shape = jax.ShapeDtypeStruct((rows, width), jnp.bfloat16)
    out_spec = pl.BlockSpec((block, width), lambda i: (i, 0))
    cost = pl.CostEstimate(
        flops=rows * width * 9 * units, bytes_accessed=rows * width * 8, transcendentals=rows * width
    )
    if send is None:
        return pl.pallas_call(
            functools.partial(update_kernel, units, chunk, scale),
            grid=(steps,),
            out_shape=out_shape,
            in_specs=in_specs,
            out_specs=out_spec,
            cost_estimate=cost,
            name="update",
        )(inv, table, g, w)
    part, rows_back = send
    n = rows_back.shape[0]
    dma = pltpu.SemaphoreType.DMA
    return pl.pallas_call(
        functools.partial(update_send_kernel, units, chunk, scale, n),
        grid=(steps,),
        out_shape=(
            out_shape,
            jax.ShapeDtypeStruct(part.shape, part.dtype),
            jax.ShapeDtypeStruct(rows_back.shape, rows_back.dtype),
        ),
        in_specs=in_specs + [pl.BlockSpec(memory_space=pl.ANY)] * 2,
        out_specs=(
            out_spec,
            pl.BlockSpec(part.shape, lambda i: (0, 0)),
            pl.BlockSpec(rows_back.shape, lambda i: (0, 0, 0)),
        ),
        scratch_shapes=[
            pltpu.VMEM((n,) + part.shape, part.dtype),
            pltpu.VMEM(rows_back.shape, rows_back.dtype),
            pltpu.VMEM(rows_back.shape, rows_back.dtype),
            dma((3,)), dma((n,)), dma((n,)), dma((n,)), dma((n,))],
        cost_estimate=cost,
        compiler_params=pltpu.CompilerParams(collective_id=2, has_side_effects=True),
        name="update_send",
    )(inv, table, g, w, part, rows_back)


def route_tables(routes, experts, capacity):
    chosen = (routes[:, :, None] == jnp.arange(experts, dtype=jnp.int32)[None, None, :]).astype(
        jnp.int32
    )
    flat_picks = chosen.reshape(-1, experts)
    before = jnp.cumsum(flat_picks, axis=0) - flat_picks
    places = jnp.sum(before * flat_picks, axis=1).reshape(routes.shape)
    slot_hit = (places[:, :, None] == jnp.arange(capacity, dtype=jnp.int32)[None, None, :]).astype(
        jnp.bfloat16
    )
    mover = chosen.astype(jnp.bfloat16)[:, :, :, None] * slot_hit[:, :, None, :]
    return (chosen.astype(jnp.float32), mover)


def on_device(
    tokens,
    cotangent,
    routes,
    router_weight,
    gate_weight,
    up_weight,
    down_weight,
    mlp_in,
    mlp_bias,
    mlp_out,
):
    experts = lax.axis_size("expert")
    groups = lax.axis_size("mp")
    tok_count = tokens.shape[0]
    capacity = 3 * tok_count // experts
    width = tokens.shape[1]
    col_width = width // groups
    mp = lax.axis_index("mp")
    me = lax.axis_index("expert")
    col_start = mp * col_width
    chosen, mover = route_tables(routes, experts, capacity)
    logits = jnp.dot(tokens, router_weight, preferred_element_type=jnp.float32)
    picked = jnp.sum(logits[:, None, :] * chosen, axis=2)
    sigmas = jax.nn.sigmoid(picked)
    denominator = jnp.sum(sigmas, axis=1, keepdims=True)
    gates = sigmas / denominator
    token_cols = lax.dynamic_slice_in_dim(tokens, col_start, col_width, 1)
    cot_cols = lax.dynamic_slice_in_dim(cotangent, col_start, col_width, 1)
    scaled_cot = (gates[:, :, None] * cot_cols.astype(jnp.float32)[:, None, :]).astype(
        jnp.bfloat16
    )
    send_x = jnp.einsum(
        "tkec,td->ecd", mover, token_cols, preferred_element_type=jnp.float32
    ).astype(jnp.bfloat16)
    send_dy = jnp.einsum(
        "tkec,tkd->ecd", mover, scaled_cot, preferred_element_type=jnp.float32
    ).astype(jnp.bfloat16)
    got = dispatch(jnp.stack([send_x, send_dy]), experts, groups)
    slots = experts * capacity
    rows_x = got[0].reshape(slots, width)
    rows_dy = got[1].reshape(slots, width)
    w_gate = gate_weight[0]
    w_up = up_weight[0]
    w_down = down_weight[0]
    hidden_units = w_gate.shape[1] * groups
    act_gate = jnp.dot(rows_x, w_gate, preferred_element_type=jnp.float32)
    act_up = jnp.dot(rows_x, w_up, preferred_element_type=jnp.float32)
    sigmoid_gate = jax.nn.sigmoid(act_gate)
    silu_gate = act_gate * sigmoid_gate
    hidden = (silu_gate * act_up).astype(jnp.bfloat16)
    partial_out = jnp.dot(hidden, w_down, preferred_element_type=jnp.float32).astype(jnp.bfloat16)
    grad_down = jnp.einsum("sf,sd->fd", hidden, rows_dy, preferred_element_type=jnp.float32)
    grad_hidden = jnp.einsum("sd,fd->sf", rows_dy, w_down, preferred_element_type=jnp.float32)
    d_gate = (grad_hidden * act_up * sigmoid_gate * (1.0 + act_gate * (1.0 - sigmoid_gate))).astype(
        jnp.bfloat16
    )
    d_up = (grad_hidden * silu_gate).astype(jnp.bfloat16)
    d_gate, d_up = lax.optimization_barrier((d_gate, d_up))
    inner = jnp.sum(grad_hidden * hidden.astype(jnp.float32), axis=1)
    grad_gate = jnp.einsum("sd,sf->df", rows_x, d_gate, preferred_element_type=jnp.float32)
    grad_up = jnp.einsum("sd,sf->df", rows_x, d_up, preferred_element_type=jnp.float32)

    norms = jnp.stack(
        [
            jnp.sum(grad_gate * grad_gate),
            jnp.sum(grad_up * grad_up),
            jnp.sum(grad_down * grad_down),
        ]
    )
    need = slots + 3
    lines = -(-need // 1024) * 8
    parcel = jnp.concatenate([inner, norms, jnp.zeros((lines * 128 - need,), jnp.float32)])
    parcels = gather_sums(parcel.reshape(lines, 128), experts, groups)
    parcels = parcels.reshape(experts, lines * 128)
    partial_out, parcels = lax.optimization_barrier((partial_out, parcels))
    total_out = lax.dynamic_slice_in_dim(partial_out, col_start, col_width, 1).astype(jnp.float32)
    for shift in range(1, groups):
        target = lax.rem(mp + shift, groups)
        piece = lax.dynamic_slice_in_dim(partial_out, target * col_width, col_width, 1)
        moved = lax.ppermute(piece, "mp", [(m, (m + shift) % groups) for m in range(groups)])
        total_out = total_out + moved.astype(jnp.float32)
    back_rows = total_out.astype(jnp.bfloat16).reshape(experts, capacity, col_width)

    norm_sums = jnp.sum(parcels[:, slots : slots + 3], axis=0)
    inner_own = lax.dynamic_slice(parcels, (0, me * capacity), (experts, capacity))

    total_count = experts * width * hidden_units
    rms = jnp.sqrt(norm_sums / total_count + EPSILON)
    table = network_table(mlp_in, mlp_bias, mlp_out)
    up_update = update(grad_up, w_up, width**0.5, rms[1], table)[None]
    down_update = update(grad_down, w_down, hidden_units**0.5, rms[2], table)[None]

    gated = jnp.sum(mover.astype(jnp.float32) * inner_own[None, None], axis=(2, 3))
    logit_grads = (gated - gates * jnp.sum(gated, axis=1, keepdims=True)) * (1.0 - sigmas)
    dense_grads = jnp.sum(logit_grads[:, :, None] * chosen, axis=1).astype(jnp.bfloat16)
    router_part = jnp.einsum("te,td->ed", dense_grads, tokens, preferred_element_type=jnp.float32)
    gate_update, router_grad, returned = update(
        grad_gate, w_gate, width**0.5, rms[0], table, send=(router_part, back_rows)
    )
    gate_update = gate_update[None]
    router_rms = jnp.sqrt(jnp.sum(router_grad * router_grad) / (width * experts) + EPSILON)
    router_update = update(router_grad, router_weight.T, width**0.5, router_rms, table).T

    routed = jnp.einsum("tkec,ecd->tkd", mover, returned, preferred_element_type=jnp.float32)
    mixed = (
        token_cols.astype(jnp.float32) + gates[:, 0:1] * routed[:, 0] + gates[:, 1:2] * routed[:, 1]
    ).astype(jnp.bfloat16)
    return (mixed, gate_update, up_update, down_update, router_update)


def solution(mesh):
    placed = (
        P("expert", None),
        P("expert", None),
        P("expert", None),
        P(),
        P("expert", None, "mp"),
        P("expert", None, "mp"),
        P("expert", "mp", None),
        P(),
        P(),
        P(),
    )
    return jax.shard_map(
        on_device,
        mesh=mesh,
        in_specs=placed,
        out_specs=(
            P("expert", "mp"),
            P("expert", None, "mp"),
            P("expert", None, "mp"),
            P("expert", "mp", None),
            P(),
        ),
        check_vma=False,
    )
```
